64 devices in a mesh: dp: 8 (over x, y, core), ep: 8 (over z).
Axes of the slice: x: 2, y: 2, z: 8, core: 2. Of those that a mesh axis runs over, the one named last changes fastest.
The devices are a block of a 4x4x8 slice.
Arguments:
- x: bfloat16 [8, 8, 256, 2048], P('dp', 'ep'), parts along dimension 0
- expert: int32 [8, 8, 256, 2], P('dp', 'ep'), parts along dimension 0
- slot: int32 [8, 8, 256, 2], P('dp', 'ep'), parts along dimension 0
- gate: float32 [8, 8, 256, 2], P('dp', 'ep'), parts along dimension 0
- w_gate: bfloat16 [8, 2048, 5632], P('ep')
- w_up: bfloat16 [8, 2048, 5632], P('ep')
- w_down: bfloat16 [8, 5632, 2048], P('ep')
Outputs:
- y: bfloat16 [8, 8, 256, 2048], P('dp', 'ep'), parts along dimension 0
There are 8 independent parts. The reference program is written for one: setup_inputs(seed, part) draws one part's arguments, and reference() takes and returns one part's arrays. A program takes and returns all parts, laid end to end along the dimension named above; an argument that names none is the same for every part.
All inputs are finite; a program needn't handle non-finite values.
Results may differ from the reference program's by a relative error of at most 0.009.
Values are sent between devices in bfloat16 or wider.
A program may use at most 768 MiB of HBM per device.

```python
import jax
import jax.numpy as jnp

MEMBERS = 8
TOKENS = 256
D = 2048
FF = 5632
TOP = 2
EXPERTS = 8
SLOTS = 5 * TOKENS * TOP // (4 * EXPERTS)


def setup_inputs(seed: int = 0, part: int = 0) -> dict:
    own, k1, k2, k3, k4, k5, k6 = jax.random.split(jax.random.key(seed), 7)
    kx, ke, kl, kg = jax.random.split(jax.random.fold_in(own, part), 4)
    devices = (1, MEMBERS)
    place = jax.random.permutation(kl, jnp.arange(EXPERTS, dtype=jnp.uint32))
    slow = ((EXPERTS + (9 * place) % EXPERTS) << ((9 * place) // EXPERTS)) // EXPERTS
    wait = (jax.random.bits(ke, (*devices, TOKENS, EXPERTS), jnp.uint32) >> 10) * slow
    expert = jnp.argsort(wait, axis=-1)[..., :TOP].astype(jnp.int32)
    chosen = jax.nn.one_hot(expert, EXPERTS, dtype=jnp.int32)
    in_line = jnp.cumsum(chosen.reshape(*devices, TOKENS * TOP, EXPERTS), axis=2) - 1
    slot = jnp.sum(in_line.reshape(chosen.shape) * chosen, axis=-1)

    def one(key, rows, columns):
        return (jax.random.normal(key, (rows, columns), jnp.float32) * rows**-0.5).astype(jnp.bfloat16)

    def weights(key, rows, columns):
        return jax.lax.map(lambda k: one(k, rows, columns), jax.random.split(key, EXPERTS))

    return {
        "x": jax.random.normal(kx, (*devices, TOKENS, D), jnp.float32).astype(jnp.bfloat16),
        "expert": expert,
        "slot": slot,
        "gate": jax.nn.softmax(jax.random.normal(kg, expert.shape, jnp.float32)),
        "w_gate": weights(k1, D, FF),
        "w_up": weights(k2, D, FF),
        "w_down": weights(k3, FF, D),
    }


def einsum(form, a, b):
    return jnp.einsum(form, a.astype(jnp.float32), b.astype(jnp.float32))


def reference(x, expert, slot, gate, w_gate, w_up, w_down):
    to_expert = jax.nn.one_hot(expert, EXPERTS, dtype=jnp.bfloat16)
    to_slot = jax.nn.one_hot(slot, SLOTS, dtype=jnp.bfloat16)
    weighted = to_expert * gate[..., None].astype(jnp.bfloat16)
    dispatch = einsum("abtke,abtkc->abtec", to_expert, to_slot).astype(jnp.bfloat16)
    combine = einsum("abtke,abtkc->abtec", weighted, to_slot).astype(jnp.bfloat16)
    z = einsum("abtec,abtd->aebcd", dispatch, x).astype(jnp.bfloat16)
    h = jax.nn.silu(einsum("aebcd,edf->aebcf", z, w_gate))
    h = (h * einsum("aebcd,edf->aebcf", z, w_up)).astype(jnp.bfloat16)
    out = einsum("aebcf,efd->aebcd", h, w_down).astype(jnp.bfloat16)
    y = einsum("abtec,aebcd->abtd", combine, out)
    return y.astype(jnp.bfloat16)
```

```python
import functools

import jax
import jax.numpy as jnp
from jax import lax
from jax.experimental import pallas as pl
from jax.experimental.pallas import tpu as pltpu
from jax.sharding import PartitionSpec as P

MESH = pl.DeviceIdType.MESH
FIRST_SHARE = 3, 5
FT = 512
NT = 256
GROUP = 2
G_SLOTS = 6
D_SLOTS = 4
BF16, F32 = jnp.bfloat16, jnp.float32


def dot(a, b):
    return jnp.dot(a, b, preferred_element_type=F32)


def kernel(
    n, slots, ra, rb,
    expert_ref, slot_ref, gate_ref, x_hbm, wg_hbm, wu_hbm, wd_hbm, y_hbm,
    x_ref, zs_a, zs_b, zr_a, zr_b, h_ref, os_a, os_b, or_a, or_b, acc, cmb_a, cmb_b, yb, g_buf, d_buf,
    x_sem, g_sem, d_sem, y_sem, zss_a, zrs_a, zss_b, zrs_b, oss_a, ors_a, oss_b, ors_b,
):
    me = lax.axis_index("ep")
    tokens, depth = x_ref.shape
    g_tiles, d_tiles = wg_hbm.shape[1] // FT, wd_hbm.shape[1] // NT
    messages, width = d_tiles // GROUP, GROUP * NT
    rows_a, rows_b = n * ra, n * rb

    def peer(d):
        return {"ep": lax.rem(me + d, n)}

    x_copy = pltpu.make_async_copy(x_hbm, x_ref, x_sem)
    x_copy.start()
    barrier = pltpu.get_barrier_semaphore()
    for d in range(1, n):
        pl.semaphore_signal(barrier, inc=1, device_id=peer(d), device_id_type=MESH)

    def g_copies(p):
        slot, tile = lax.rem(p, G_SLOTS), lax.rem(p, g_tiles)
        cols = pl.ds(pl.multiple_of(tile * FT, FT), FT)
        return [
            pltpu.make_async_copy(w.at[:, cols], g_buf.at[slot, i], g_sem.at[slot, i])
            for i, w in enumerate((wg_hbm, wu_hbm))
        ]

    def d_copy(p):
        slot, tile = lax.rem(p, D_SLOTS), lax.rem(p, d_tiles)
        cols = pl.ds(pl.multiple_of(tile * NT, NT), NT)
        return pltpu.make_async_copy(wd_hbm.at[:, cols], d_buf.at[slot], d_sem.at[slot])

    @pl.loop(0, G_SLOTS)
    def _(p):
        for c in g_copies(p):
            c.start()

    @pl.loop(0, D_SLOTS)
    def _(p):
        d_copy(p).start()

    rel = expert_ref[...] - me
    rel = jnp.where(rel < 0, rel + n, rel)
    slot = slot_ref[...]
    code_a = jnp.where(slot < ra, rel * ra + slot, -1)
    code_b = jnp.where((slot >= ra) & (slot < slots), rel * rb + slot - ra, -1)

    def picks(code, rows):
        row = lax.broadcasted_iota(jnp.int32, (rows, tokens), 0)
        return row == code[0:1, :], row == code[1:2, :]

    x_copy.wait()
    x = x_ref[...]
    for code, rows, r, zs, zr in (
        (code_a, rows_a, ra, zs_a, zr_a),
        (code_b, rows_b, rb, zs_b, zr_b),
    ):
        p0, p1 = picks(code, rows)
        z = dot((p0 | p1).astype(F32).astype(BF16), x).astype(BF16)
        zr[0:r, :] = z[0:r]
        zs[r:, :] = z[r:]

    pl.semaphore_wait(barrier, n - 1)

    far_first = sorted(range(1, n), key=lambda d: (-min(d, n - d), d))

    def z_copy(d, r, zs, zr, send, recv):
        rows = pl.ds(d * r, r)
        return pltpu.make_async_remote_copy(
            src_ref=zs.at[rows], dst_ref=zr.at[rows], send_sem=send.at[d], recv_sem=recv.at[d],
            device_id=peer(d), device_id_type=MESH,
        )

    z_a = [z_copy(d, ra, zs_a, zr_a, zss_a, zrs_a) for d in far_first]
    z_b = [z_copy(d, rb, zs_b, zr_b, zss_b, zrs_b) for d in far_first]
    for c in z_a + z_b:
        c.start()

    gate = gate_ref[...].astype(BF16).astype(F32)
    for code, rows, cmb in ((code_a, rows_a, cmb_a), (code_b, rows_b, cmb_b)):
        p0, p1 = picks(code, rows)
        w = jnp.where(p0, gate[0:1, :], jnp.where(p1, gate[1:2, :], 0.0))
        cmb[...] = w.T.astype(BF16)

    def up(zr, rows, start, stop, fresh):
        @pl.loop(0, g_tiles)
        def _(i):
            p = start + i
            slot, tile = lax.rem(p, G_SLOTS), lax.rem(p, g_tiles)

            @pl.when(p >= fresh)
            def _():
                for c in g_copies(p):
                    c.wait()

            z = zr[...]
            g, u = dot(z, g_buf[slot, 0]), dot(z, g_buf[slot, 1])
            h_ref[0:rows, pl.ds(pl.multiple_of(tile * FT, FT), FT)] = (jax.nn.silu(g) * u).astype(BF16)

            @pl.when(p + G_SLOTS < stop)
            def _():
                for c in g_copies(p + G_SLOTS):
                    c.start()

    def o_copy(m, d, r, os, orr, send, recv):
        rows = pl.ds(d * r, r)
        return pltpu.make_async_remote_copy(
            src_ref=os.at[m, rows], dst_ref=orr.at[m, rows], send_sem=send.at[m, d], recv_sem=recv.at[m, d],
            device_id=peer(n - d), device_id_type=MESH,
        )

    def down(rows, r, os, orr, send, recv, start, stop, fresh):
        @pl.loop(0, messages)
        def _(i):
            m = lax.rem(start // GROUP + i, messages)
            for j in range(GROUP):
                p = start + GROUP * i + j
                slot = lax.rem(p, D_SLOTS)

                @pl.when(p >= fresh)
                def _():
                    d_copy(p).wait()

                o = dot(h_ref[0:rows, :], d_buf[slot]).astype(BF16)
                orr[m, 0:r, j * NT : (j + 1) * NT] = o[0:r]
                os[m, r:, j * NT : (j + 1) * NT] = o[r:]

                @pl.when(p + D_SLOTS < stop)
                def _():
                    d_copy(p + D_SLOTS).start()

            for d in far_first:
                o_copy(m, d, r, os, orr, send, recv).start()

    for c in z_a:
        c.wait_recv()
    up(zr_a, rows_a, 0, g_tiles, 0)
    down(rows_a, ra, os_a, or_a, oss_a, ors_a, 0, d_tiles, 0)
    for c in z_b:
        c.wait_recv()
    up(zr_b, rows_b, g_tiles - G_SLOTS, 2 * g_tiles - G_SLOTS, g_tiles)
    down(rows_b, rb, os_b, or_b, oss_b, ors_b, d_tiles - D_SLOTS, 2 * d_tiles - D_SLOTS, d_tiles)

    @pl.loop(0, messages)
    def _(m):
        for d in far_first:
            o_copy(m, d, ra, os_a, or_a, oss_a, ors_a).wait_recv()
        acc[m] = dot(cmb_a[...], or_a[m])

    def y_copy(m):
        cols = pl.ds(pl.multiple_of(m * width, width), width)
        return pltpu.make_async_copy(yb.at[m], y_hbm.at[:, cols], y_sem.at[m])

    @pl.loop(0, messages)
    def _(i):
        m = lax.rem((d_tiles - D_SLOTS) // GROUP + i, messages)
        for d in far_first:
            o_copy(m, d, rb, os_b, or_b, oss_b, ors_b).wait_recv()
        yb[m] = (acc[m] + dot(cmb_b[...], or_b[m])).astype(BF16)
        y_copy(m).start()

    for c in z_a + z_b:
        c.wait_send()

    @pl.loop(0, messages)
    def _(m):
        for d in far_first:
            o_copy(m, d, ra, os_a, or_a, oss_a, ors_a).wait_send()
            o_copy(m, d, rb, os_b, or_b, oss_b, ors_b).wait_send()
        y_copy(m).wait()


def solution(mesh):
    n = mesh.shape["ep"]

    def step(x, expert, slot, gate, w_gate, w_up, w_down):
        tokens, depth = x.shape[2:]
        top, hidden = expert.shape[3], w_gate.shape[2]
        slots = 5 * tokens * top // (4 * n)
        ra = slots * FIRST_SHARE[0] // FIRST_SHARE[1]
        rb = slots - ra
        messages, width = depth // (GROUP * NT), GROUP * NT
        vmem, any_space = pl.BlockSpec(memory_space=pltpu.VMEM), pl.BlockSpec(memory_space=pl.ANY)
        dma = pltpu.SemaphoreType.DMA
        y = pl.pallas_call(
            functools.partial(kernel, n, slots, ra, rb),
            out_shape=jax.ShapeDtypeStruct((tokens, depth), BF16),
            in_specs=[vmem] * 3 + [any_space] * 4,
            out_specs=any_space,
            scratch_shapes=[
                pltpu.VMEM((tokens, depth), BF16),
                pltpu.VMEM((n * ra, depth), BF16),
                pltpu.VMEM((n * rb, depth), BF16),
                pltpu.VMEM((n * ra, depth), BF16),
                pltpu.VMEM((n * rb, depth), BF16),
                pltpu.VMEM((n * max(ra, rb), hidden), BF16),
                pltpu.VMEM((messages, n * ra, width), BF16),
                pltpu.VMEM((messages, n * rb, width), BF16),
                pltpu.VMEM((messages, n * ra, width), BF16),
                pltpu.VMEM((messages, n * rb, width), BF16),
                pltpu.VMEM((messages, tokens, width), F32),
                pltpu.VMEM((tokens, n * ra), BF16),
                pltpu.VMEM((tokens, n * rb), BF16),
                pltpu.VMEM((messages, tokens, width), BF16),
                pltpu.VMEM((G_SLOTS, 2, depth, FT), BF16),
                pltpu.VMEM((D_SLOTS, hidden, NT), BF16),
                dma,
                dma((G_SLOTS, 2)),
                dma((D_SLOTS,)),
                dma((messages,)),
                dma((n,)),
                dma((n,)),
                dma((n,)),
                dma((n,)),
                dma((messages, n)),
                dma((messages, n)),
                dma((messages, n)),
                dma((messages, n)),
            ],
            compiler_params=pltpu.CompilerParams(
                collective_id=0, has_side_effects=True, vmem_limit_bytes=67_043_328
            ),
            name="moe",
        )(expert[0, 0].T, slot[0, 0].T, gate[0, 0].T, x[0, 0], w_gate[0], w_up[0], w_down[0])
        return y[None, None]

    tokens_spec, weights_spec = P("dp", "ep"), P("ep")
    return jax.shard_map(
        step,
        mesh=mesh,
        in_specs=(tokens_spec,) * 4 + (weights_spec,) * 3,
        out_specs=tokens_spec,
        check_vma=False,
    )
```
